128 devices in a mesh: gx: 16 (over z, y_hi, core), gy: 8 (over y_lo, x).
Axes of the slice: x: 4, y: 4 (y_hi: 2, y_lo: 2; y = y_hi * 2 + y_lo), z: 4, core: 2. Of those that a mesh axis runs over, the one named last changes fastest.
Arguments:
- density: float32 [256, 256, 256], P('gx', 'gy'), may hold values from 0.05 to 2
Outputs:
- potential: float32 [256, 256, 256], P('gx', 'gy')
- energy: float32 [], replicated
The draws below stay inside these ranges and needn't reach their ends.
All inputs are finite; a program needn't handle non-finite values.
Results may differ from the reference program's by a relative error of at most 0.00005.
Values sent between devices are 32-bit elements.
No kernel may reach another device: no remote copies, remote signals or barrier semaphores. Data moves between devices by JAX's collectives and lax.ppermute only.
A program may use at most 64 MiB of HBM per device.

```python
import math
import jax
import jax.numpy as jnp

NX = 256
NY = 256
NZ = 256


def block_scale(stream_key, dims, split, least, high):
    gain = 1.0
    for position, blocks in split:
        heights = jax.random.uniform(jax.random.fold_in(jax.random.fold_in(stream_key, 6), position), (blocks,), jnp.float32, least / len(split), high / len(split))
        gain = gain * jnp.repeat(jnp.exp(heights), dims[position] // blocks).reshape((-1,) + (1,) * (len(dims) - 1 - position))
    return gain


def setup_inputs(seed: int = 0) -> dict:
    streams_of = jax.random.split(jax.random.key(seed), 2)
    density = jnp.clip(jnp.exp(math.log(2.0) - 3.6888794 * jax.random.uniform(streams_of[0], (NX, NY, NZ), jnp.float32) ** block_scale(streams_of[0], (NX, NY, NZ), ((0, 16), (1, 8)), -0.2, 0.2)), 0.05, 2.0)
    return dict(density=density)


spacing = 1.0
pbe_kappa = 0.804
pbe_mu = 0.2195149727645171
pbe_beta = 0.06672455060314922
pbe_gamma = 0.031090690869654894
pw_coef = 0.0310907
pw_alpha = 0.2137
pw_first = 7.5957
pw_second = 3.5876
pw_third = 1.6382
pw_fourth = 0.49294

def xc_energy(electrons, grad_sq):
    k_fermi = jnp.cbrt(3.0 * math.pi ** 2 * electrons)
    exch_unif = -0.75 * k_fermi / math.pi
    s_square = grad_sq / (4.0 * k_fermi ** 2 * electrons ** 2)
    enhance = 1.0 + pbe_kappa - pbe_kappa / (1.0 + pbe_mu * s_square / pbe_kappa)
    wigner = jnp.cbrt(3.0 / (4.0 * math.pi * electrons))
    root_rs = jnp.sqrt(wigner)
    series = 2.0 * pw_coef * (pw_first * root_rs + pw_second * wigner + pw_third * wigner * root_rs + pw_fourth * wigner ** 2)
    corr_unif = -2.0 * pw_coef * (1.0 + pw_alpha * wigner) * jnp.log(1.0 + 1.0 / series)
    screen_sq = 4.0 * k_fermi / math.pi
    t_square = grad_sq / (4.0 * screen_sq * electrons ** 2)
    factor = pbe_beta / pbe_gamma / jnp.expm1(-corr_unif / pbe_gamma)
    scaled = factor * t_square
    gradient_term = pbe_gamma * jnp.log(1.0 + pbe_beta / pbe_gamma * t_square * (1.0 + scaled) / (1.0 + scaled + scaled ** 2))
    return electrons * (exch_unif * enhance + corr_unif + gradient_term)

def summed_energy(electrons, grad_sq):
    return jnp.sum(xc_energy(electrons, grad_sq))

def wavenum(count):
    index = jnp.arange(count, dtype=jnp.int32)
    signed = jnp.where(index < count // 2, index, index - count)
    signed = jnp.where(index == count // 2, 0, signed)
    return signed.astype(jnp.float32) * (2.0 * math.pi / (count * spacing))

def reference(density):
    spectrum = jnp.fft.fftn(density)
    waves = (wavenum(NX)[:, None, None], wavenum(NY)[None, :, None], wavenum(NZ)[None, None, :])
    gradients = [jnp.real(jnp.fft.ifftn(1j * wavevec * spectrum)) for wavevec in waves]
    grad_sq = gradients[0] ** 2 + gradients[1] ** 2 + gradients[2] ** 2
    energy_sum, partials = jax.value_and_grad(summed_energy, argnums=(0, 1))(density, grad_sq)
    d_dens, d_grad = partials
    flux_spec = 1j * waves[0] * jnp.fft.fftn(2.0 * d_grad * gradients[0])
    flux_spec = flux_spec + 1j * waves[1] * jnp.fft.fftn(2.0 * d_grad * gradients[1])
    flux_spec = flux_spec + 1j * waves[2] * jnp.fft.fftn(2.0 * d_grad * gradients[2])
    divergence = jnp.real(jnp.fft.ifftn(flux_spec))
    potential = d_dens - divergence
    energy = energy_sum / (NX * NY * NZ)
    return (potential, energy)
```

```python
import functools
import math

import jax
import jax.numpy as jnp
import numpy as np
from jax import lax
from jax.experimental import pallas as pl
from jax.experimental.pallas import tpu as pltpu
from jax.sharding import PartitionSpec as P

AXES = ("gx", "gy")
LANES = 128
VIEW = 8
highest = lax.Precision.HIGHEST

pbe_kappa = 0.804
pbe_mu = 0.2195149727645171
pbe_beta = 0.06672455060314922
pbe_gamma = 0.031090690869654894
pw_coef = 0.0310907
pw_alpha = 0.2137
pw_first = 7.5957
pw_second = 3.5876
pw_third = 1.6382
pw_fourth = 0.49294

fermi_scale = (3.0 * math.pi**2) ** (1.0 / 3.0)
exch_scale = 0.75 * fermi_scale / math.pi
s_scale = 1.0 / (4.0 * fermi_scale**2)
t_scale = math.pi / (16.0 * fermi_scale)
rs_scale = (3.0 / (4.0 * math.pi)) ** (1.0 / 3.0)
beta_gamma = pbe_beta / pbe_gamma


def deriv_matrix(count):
    index = np.arange(count)
    signed = np.where(index < count // 2, index, index - count)
    signed = np.where(index == count // 2, 0, signed)
    waves = signed * (2.0 * math.pi / count)
    phase = (index[:, None] * index[None, :] % count) * (2.0 * math.pi / count)
    cosine, sine = np.cos(phase), np.sin(phase)
    return ((cosine * waves) @ sine - (sine * waves) @ cosine) / count


def mul(left, right):
    return jnp.dot(left, right, precision=highest, preferred_element_type=jnp.float32)


def pbe(n, g):
    v = jnp.exp2(jnp.log2(n) * (-1.0 / 3.0))
    v = v * (4.0 / 3.0 - (1.0 / 3.0) * n * v * v * v)
    v2 = v * v
    v4 = v2 * v2
    u = n * v2
    g4 = g * v4
    s2 = s_scale * g4 * v4
    t2 = t_scale * g4 * v2 * v
    damp = 1.0 / (1.0 + (pbe_mu / pbe_kappa) * s2)
    ex = -exch_scale * u
    fx = 1.0 + pbe_kappa - pbe_kappa * damp
    slope = pbe_mu * damp * damp
    rs = rs_scale * v
    root = jnp.sqrt(rs)
    series = (2.0 * pw_coef) * root * (
        pw_first + root * (pw_second + root * (pw_third + root * pw_fourth))
    )
    dseries = (2.0 * pw_coef) * root * (
        0.5 * pw_first + root * (pw_second + root * (1.5 * pw_third + root * (2.0 * pw_fourth)))
    )
    inverse = 1.0 / series
    logarithm = jnp.log(1.0 + inverse)
    front = (-2.0 * pw_coef) * (1.0 + pw_alpha * rs)
    ec = front * logarithm
    rs_dec = (-2.0 * pw_coef * pw_alpha) * rs * logarithm - front * dseries * inverse / (
        1.0 + series
    )
    n_dec = (-1.0 / 3.0) * rs_dec
    below = 1.0 / (jnp.exp(ec * (-1.0 / pbe_gamma)) - 1.0)
    factor = beta_gamma * below
    n_dfactor = factor * (1.0 + below) * (1.0 / pbe_gamma) * n_dec
    y = factor * t2
    base = 1.0 + y + y * y
    top = base + beta_gamma * t2 * (1.0 + y)
    both = 1.0 / (base * top)
    h = pbe_gamma * jnp.log(top * top * both)
    energy = ex * fx + ec + h
    d_grad = v4 * (
        (-exch_scale * s_scale) * slope + (pbe_beta * t_scale) * (1.0 + 2.0 * y) * both
    )
    n_dh = pbe_beta * both * (
        (-7.0 / 3.0) * t2 * (1.0 + 2.0 * y) - t2 * t2 * y * (2.0 + y) * n_dfactor
    )
    d_dens = energy + ex * ((1.0 / 3.0) * fx - (8.0 / 3.0) * slope * s2) + n_dec + n_dh
    return n * energy, d_dens, d_grad


def quarter_swap(parts):
    quarter = lax.broadcasted_iota(jnp.int32, parts[0].shape, parts[0].ndim - 1) // 32
    for bit in (1, 2):
        upper = (quarter & bit) != 0
        swapped = list(parts)
        for low in range(4):
            if low & bit:
                continue
            high = low | bit
            first, second = parts[low], parts[high]
            axis = first.ndim - 1
            swapped[low] = jnp.where(upper, pltpu.roll(second, 32 * bit, axis), first)
            swapped[high] = jnp.where(upper, second, pltpu.roll(first, LANES - 32 * bit, axis))
        parts = swapped
    return parts


def first_kernel(density_ref, deriv_ref, send_ref):
    lines = density_ref[...].reshape(-1, density_ref.shape[-1])
    turned = lines.T
    slopes = mul(deriv_ref[...], turned)
    rows = 2 * VIEW
    for field, values in enumerate((turned, slopes)):
        for plane in range(2):
            for part in range(4):
                send_ref[pl.ds(VIEW * field + 4 * plane + part, LANES, stride=rows), :] = values[
                    LANES * plane : LANES * (plane + 1), LANES * part : LANES * (part + 1)
                ]


def middle_kernel(
    got_ref, deriv_x_ref, deriv_y_ref, send_ref, dens_ref, grad_z_ref, grad_x_ref, grad_y_ref
):
    rows = 2 * VIEW
    for a in range(16):
        for field, ref in enumerate((dens_ref, grad_z_ref)):
            for half in range(2):
                parts = []
                for quarter in range(4):
                    start = ((a * 2 + half) * 4 + quarter) * rows + VIEW * field
                    parts.append(got_ref[start : start + VIEW, :])
                for quarter, part in enumerate(quarter_swap(parts)):
                    start = (a * 4 + quarter) * VIEW
                    ref[start : start + VIEW, LANES * half : LANES * (half + 1)] = part
    grad_x_ref[...] = mul(deriv_x_ref[...], dens_ref[...])
    grad_y_ref[...] = mul(dens_ref[...], deriv_y_ref[...])

    def evaluate(step, total):
        block = pl.ds(pl.multiple_of(step * 32, 32), 32)
        n = dens_ref[block, :]
        gx, gy, gz = grad_x_ref[block, :], grad_y_ref[block, :], grad_z_ref[block, :]
        f, d_dens, d_grad = pbe(n, gx * gx + gy * gy + gz * gz)
        twice = 2.0 * d_grad
        grad_x_ref[block, :] = twice * gx
        grad_y_ref[block, :] = twice * gy
        grad_z_ref[block, :] = twice * gz
        dens_ref[block, :] = d_dens
        return total + f

    total = lax.fori_loop(0, 16, evaluate, jnp.zeros((32, 256), jnp.float32))
    dens_ref[...] = (
        dens_ref[...]
        - mul(deriv_x_ref[...], grad_x_ref[...])
        - mul(grad_y_ref[...], deriv_y_ref[...])
    )
    for a in range(16):
        for field, ref in enumerate((dens_ref, grad_z_ref)):
            for half in range(2):
                parts = []
                for quarter in range(4):
                    start = (a * 4 + quarter) * VIEW
                    parts.append(ref[start : start + VIEW, LANES * half : LANES * (half + 1)])
                for quarter, part in enumerate(quarter_swap(parts)):
                    start = ((a * 2 + half) * 4 + quarter) * (rows + 1) + VIEW * field
                    send_ref[start : start + VIEW, :] = part
    summed = jnp.sum(total[:, :LANES] + total[:, LANES:], axis=0, keepdims=True)
    send_ref[pl.ds(rows, LANES, stride=rows + 1), :] = jnp.broadcast_to(summed, (LANES, LANES))


def last_kernel(cells, got_ref, deriv_ref, potential_ref, energy_ref):
    rows = 2 * VIEW + 1

    def gather(field):
        return jnp.concatenate(
            [
                jnp.concatenate(
                    [
                        got_ref[pl.ds(VIEW * field + 4 * plane + part, LANES, stride=rows), :]
                        for part in range(4)
                    ],
                    axis=1,
                )
                for plane in range(2)
            ],
            axis=0,
        )

    turned = gather(0) - mul(deriv_ref[...], gather(1))
    potential_ref[...] = turned.T.reshape(potential_ref.shape)
    energy_ref[0, 0] = jnp.sum(got_ref[pl.ds(rows - 1, LANES, stride=rows), :]) / cells


def in_vmem(count):
    return [pl.BlockSpec(memory_space=pltpu.VMEM)] * count


def exchange(values):
    return lax.all_to_all(values, AXES, split_axis=0, concat_axis=0, tiled=True)


def body(cells, density):
    count = density.shape[-1]
    deriv = deriv_matrix(count)
    row = np.arange(2 * count)
    plane = (row // 4) % 2
    cell = 16 * (row // 32) + 4 * (row % 4) + (row // 8) % 4
    double = np.where(plane[:, None] == plane[None, :], deriv[cell[:, None], cell[None, :]], 0.0)
    deriv_z = jnp.asarray(deriv, jnp.float32)
    deriv_y = jnp.asarray(deriv.T, jnp.float32)
    deriv_x = jnp.asarray(double, jnp.float32)

    send = pl.pallas_call(
        first_kernel,
        out_shape=jax.ShapeDtypeStruct((2048, LANES), jnp.float32),
        in_specs=in_vmem(2),
        out_specs=pl.BlockSpec(memory_space=pltpu.VMEM),
    )(density, deriv_z)
    got = exchange(send.reshape(LANES, 16, LANES)).reshape(2048, LANES)
    send = pl.pallas_call(
        middle_kernel,
        out_shape=jax.ShapeDtypeStruct((17 * LANES, LANES), jnp.float32),
        in_specs=in_vmem(3),
        out_specs=pl.BlockSpec(memory_space=pltpu.VMEM),
        scratch_shapes=[pltpu.VMEM((512, 256), jnp.float32)] * 4,
    )(got, deriv_x, deriv_y)
    got = exchange(send.reshape(LANES, 1, 17 * LANES)).reshape(17 * LANES, LANES)
    potential, energy = pl.pallas_call(
        functools.partial(last_kernel, float(cells)),
        out_shape=(
            jax.ShapeDtypeStruct(density.shape, jnp.float32),
            jax.ShapeDtypeStruct((1, 1), jnp.float32),
        ),
        in_specs=in_vmem(2),
        out_specs=(
            pl.BlockSpec(memory_space=pltpu.VMEM),
            pl.BlockSpec(memory_space=pltpu.SMEM),
        ),
    )(got, deriv_z)
    return potential, energy.reshape(())


def solution(mesh):
    return jax.shard_map(
        functools.partial(body, 256**3),
        mesh=mesh,
        in_specs=(P("gx", "gy", None),),
        out_specs=(P("gx", "gy", None), P()),
        check_vma=False,
    )
```

```python
import functools
import math

import jax
import jax.numpy as jnp
import numpy as np
from jax import lax
from jax.experimental import pallas as pl
from jax.experimental.pallas import tpu as pltpu
from jax.sharding import PartitionSpec as P

AXES = ("gx", "gy")
LANES = 128
VIEW = 8
GROUP = 4
BLOCK = 32

pbe_kappa = 0.804
pbe_mu = 0.2195149727645171
pbe_beta = 0.06672455060314922
pbe_gamma = 0.031090690869654894
pw_coef = 0.0310907
pw_alpha = 0.2137
pw_first = 7.5957
pw_second = 3.5876
pw_third = 1.6382
pw_fourth = 0.49294

fermi_scale = (3.0 * math.pi**2) ** (1.0 / 3.0)
exch_scale = 0.75 * fermi_scale / math.pi
s_scale = 1.0 / (4.0 * fermi_scale**2)
t_scale = math.pi / (16.0 * fermi_scale)
rs_scale = (3.0 / (4.0 * math.pi)) ** (1.0 / 3.0)
root_slope = -1.0 / (6.0 * math.log(2.0))
root_shift = 0.5 * math.log2(rs_scale)
damping_scale = pbe_mu / pbe_kappa * s_scale / rs_scale**8
tau_scale = pbe_beta / pbe_gamma * t_scale / rs_scale**7
slope_scale = -2.0 * exch_scale * s_scale * pbe_mu / rs_scale**4
weight_scale = 2.0 * pbe_beta * t_scale / rs_scale**4
pw = [2.0 * pw_coef * factor for factor in (pw_first, pw_second, pw_third, pw_fourth)]


def deriv_matrix(count):
    index = np.arange(count)
    signed = np.where(index < count // 2, index, index - count)
    signed = np.where(index == count // 2, 0, signed)
    waves = signed * (2.0 * math.pi / count)
    phase = (index[:, None] * index[None, :] % count) * (2.0 * math.pi / count)
    cosine, sine = np.cos(phase), np.sin(phase)
    return ((cosine * waves) @ sine - (sine * waves) @ cosine) / count


def halves(values):
    high = values.astype(jnp.bfloat16)
    return high, (values - high.astype(jnp.float32)).astype(jnp.bfloat16)


def mul(left, right):
    def dot(first, second):
        return jnp.dot(first, second, preferred_element_type=jnp.float32)

    return dot(left[0], right[0]) + dot(left[1], right[0]) + dot(left[0], right[1])


def pbe(n, g):
    root = jnp.exp2(jnp.log(n) * root_slope + root_shift)
    rs = root * root
    rs2 = rs * rs
    rs4 = rs2 * rs2
    scaled = g * rs4
    damping = 1.0 + damping_scale * (scaled * rs4)
    tau = tau_scale * (scaled * (rs2 * rs))
    ex = (-exch_scale / rs_scale**2) * (n * rs2)
    series = root * (pw[0] + root * (pw[1] + root * (pw[2] + root * pw[3])))
    third = root * (
        pw[0] / 6 + root * (pw[1] / 3 + root * (pw[2] / 2 + root * (pw[3] / 1.5)))
    )
    outer = 1.0 + series
    product = series * outer
    inverse = 1.0 / (product * damping)
    damp = product * inverse
    fraction = damping * inverse
    logarithm = jnp.log(1.0 + outer * fraction)
    curved = (-2.0 * pw_coef * pw_alpha) * rs
    front = curved - 2.0 * pw_coef
    ec = front * logarithm
    n_dec = front * (third * fraction) - (curved * (1.0 / 3.0)) * logarithm
    grown = jnp.exp2(ec * (-1.0 / (pbe_gamma * math.log(2.0))))
    m = grown - 1.0
    m2 = m * m
    cross = tau * m
    tau2 = tau * tau
    near = m + tau
    base = m2 + cross + tau2
    top = base + cross * near
    both = 1.0 / (base * top)
    rest = ec + pbe_gamma * jnp.log(top * (top * both))
    damp2 = damp * damp
    energy = ex * ((1.0 + pbe_kappa) - pbe_kappa * damp) + rest
    weight = (near + tau) * (m2 * m)
    twice = rs4 * (slope_scale * damp2 + (weight_scale * weight) * both)
    n_dh = (tau * both) * (
        (-7.0 / 3.0 * pbe_gamma) * weight - tau2 * ((near + m) * (grown * n_dec))
    )
    d_dens = (
        ex
        * (
            (4.0 / 3.0) * (1.0 + pbe_kappa)
            + damp * ((-4.0 * pbe_kappa) + (8.0 / 3.0 * pbe_kappa) * damp)
        )
        + (rest + n_dec)
        + n_dh
    )
    return n * energy, d_dens, twice


def mix(parts, odd, upper):
    pairs = [jnp.where(odd, parts[(1 - t) % 4], parts[-t % 4]) for t in range(4)]
    return [jnp.where(upper, pairs[(t + 2) % 4], pairs[t]) for t in range(4)]


def swap_rows(first, second, below):
    return (
        jnp.where(below, pltpu.roll(second, 4, 0), first),
        jnp.where(below, second, pltpu.roll(first, 4, 0)),
    )


def masks():
    lane = lax.broadcasted_iota(jnp.int32, (VIEW, LANES), 1)
    row = lax.broadcasted_iota(jnp.int32, (VIEW, LANES), 0)
    return (lane & 32) != 0, (lane & 64) != 0, (row & 4) != 0


def turn():
    return lax.rem(lax.axis_index("gy"), 4)


def first_kernel(density_hbm, deriv_hbm, send_ref, density_ref, deriv_ref, sems):
    copies = [
        pltpu.make_async_copy(density_hbm, density_ref, sems.at[0]),
        pltpu.make_async_copy(deriv_hbm, deriv_ref, sems.at[1]),
    ]
    for copy in copies:
        copy.start()
    back = 4 - turn()
    copies[0].wait()
    lines = jnp.concatenate(
        [density_ref[4 * (place // 4) + lax.rem(place % 4 + back, 4)] for place in range(16)]
    )
    turned = lines.T
    copies[1].wait()
    slopes = mul((deriv_ref[0], deriv_ref[1]), halves(turned))
    rows = 2 * VIEW
    for field, values in enumerate((turned, slopes)):
        for plane in range(2):
            for part in range(4):
                send_ref[pl.ds(VIEW * field + 4 * plane + part, LANES, stride=rows), :] = values[
                    LANES * plane : LANES * (plane + 1), LANES * part : LANES * (part + 1)
                ]


def middle_kernel(
    got_ref, deriv_x_ref, deriv_y_ref, send_ref, dens_ref, grad_z_ref, grad_x_ref, grad_y_ref
):
    rows = 2 * VIEW
    odd, upper, below = masks()

    def receive(step, carry):
        for inner in range(GROUP):
            a = step * GROUP + inner
            for field, ref in enumerate((dens_ref, grad_z_ref)):
                for half in range(2):
                    parts = []
                    for quarter in range(4):
                        start = a * (8 * rows) + ((half * 4 + quarter) * rows + VIEW * field)
                        parts.append(got_ref[pl.ds(pl.multiple_of(start, VIEW), VIEW), :])
                    parts = [
                        pltpu.roll(part, LANES - 32 * t, 1) if t else part
                        for t, part in enumerate(mix(parts, odd, upper))
                    ]
                    for pair in range(2):
                        start = pl.multiple_of(a * 16 + pair * VIEW, VIEW)
                        planes = swap_rows(parts[2 * pair], parts[2 * pair + 1], below)
                        for plane in range(2):
                            ref[
                                plane, pl.ds(start, VIEW), LANES * half : LANES * (half + 1)
                            ] = planes[plane]
        return carry

    lax.fori_loop(0, 16 // GROUP, receive, 0)
    deriv_x = deriv_x_ref[0], deriv_x_ref[1]
    deriv_y = deriv_y_ref[0], deriv_y_ref[1]
    for plane in range(2):
        dens = halves(dens_ref[plane])
        grad_x_ref[plane] = mul(deriv_x, dens)
        grad_y_ref[plane] = mul(dens, deriv_y)

    def evaluate(step, total):
        plane, start = lax.div(step, 256 // BLOCK), lax.rem(step, 256 // BLOCK) * BLOCK
        block = plane, pl.ds(pl.multiple_of(start, BLOCK), BLOCK)
        n = dens_ref[block]
        gx, gy, gz = grad_x_ref[block], grad_y_ref[block], grad_z_ref[block]
        f, d_dens, twice = pbe(n, gx * gx + gy * gy + gz * gz)
        grad_x_ref[block] = twice * gx
        grad_y_ref[block] = twice * gy
        grad_z_ref[block] = twice * gz
        dens_ref[block] = d_dens
        return total + f

    total = lax.fori_loop(0, 512 // BLOCK, evaluate, jnp.zeros((BLOCK, 256), jnp.float32))
    for plane in range(2):
        dens_ref[plane] = (
            dens_ref[plane]
            - mul(deriv_x, halves(grad_x_ref[plane]))
            - mul(halves(grad_y_ref[plane]), deriv_y)
        )

    def give(step, carry):
        for inner in range(GROUP):
            a = step * GROUP + inner
            for field, ref in enumerate((dens_ref, grad_z_ref)):
                for half in range(2):
                    parts = []
                    for pair in range(2):
                        start = pl.multiple_of(a * 16 + pair * VIEW, VIEW)
                        planes = [
                            ref[plane, pl.ds(start, VIEW), LANES * half : LANES * (half + 1)]
                            for plane in range(2)
                        ]
                        parts.extend(swap_rows(*planes, below))
                    parts = [
                        pltpu.roll(part, 32 * t, 1) if t else part for t, part in enumerate(parts)
                    ]
                    for quarter, part in enumerate(mix(parts, odd, upper)):
                        start = (half * 4 + quarter) * (rows + 1) + VIEW * field
                        send_ref[pl.ds(a * (8 * rows + 8) + start, VIEW), :] = part
        return carry

    lax.fori_loop(0, 16 // GROUP, give, 0)
    summed = jnp.sum(total[:, :LANES] + total[:, LANES:], axis=0, keepdims=True)
    send_ref[pl.ds(rows, LANES, stride=rows + 1), :] = jnp.broadcast_to(summed, (LANES, LANES))


def last_kernel(cells, got_ref, deriv_ref, potential_ref, energy_ref):
    rows = 2 * VIEW + 1
    back = 4 - turn()

    def gather(field):
        return jnp.concatenate(
            [
                jnp.concatenate(
                    [
                        got_ref[pl.ds(VIEW * field + 4 * plane + part, LANES, stride=rows), :]
                        for part in range(4)
                    ],
                    axis=1,
                )
                for plane in range(2)
            ],
            axis=0,
        )

    turned = gather(0) - mul((deriv_ref[0], deriv_ref[1]), halves(gather(1)))
    lines = turned.T
    for place in range(16):
        potential_ref[4 * (place // 4) + lax.rem(place % 4 + back, 4)] = lines[
            32 * place : 32 * (place + 1)
        ]
    energy_ref[0, 0] = jnp.sum(got_ref[pl.ds(rows - 1, LANES, stride=rows), :]) / cells


def params(megabytes):
    return pltpu.CompilerParams(vmem_limit_bytes=megabytes << 20)


def in_vmem(count):
    return [pl.BlockSpec(memory_space=pltpu.VMEM)] * count


def far(values):
    return pltpu.with_memory_space_constraint(values, pltpu.HBM)


def exchange(values):
    return lax.all_to_all(values, AXES, split_axis=0, concat_axis=0, tiled=True)


def pair(matrix):
    high = matrix.astype(jnp.bfloat16)
    low = (matrix - high.astype(np.float64)).astype(jnp.bfloat16)
    return jnp.asarray(np.stack([high, low]))


def body(cells, density):
    count = density.shape[-1]
    deriv = deriv_matrix(count)
    row = np.arange(count)
    cell = 16 * (row // 16) + 4 * (row % 4) + (row // 4) % 4
    deriv_z = pair(deriv)
    deriv_y = pair(deriv.T)
    deriv_x = pair(deriv[cell[:, None], cell[None, :]])

    send = pl.pallas_call(
        first_kernel,
        out_shape=jax.ShapeDtypeStruct((2048, LANES), jnp.float32),
        in_specs=[pl.BlockSpec(memory_space=pltpu.HBM)] * 2,
        out_specs=pl.BlockSpec(memory_space=pltpu.VMEM),
        scratch_shapes=[
            pltpu.VMEM(density.shape, jnp.float32),
            pltpu.VMEM((2, count, count), jnp.bfloat16),
            pltpu.SemaphoreType.DMA((2,)),
        ],
        compiler_params=params(12),
    )(far(density), far(deriv_z))
    got = exchange(send.reshape(LANES, 16, LANES)).reshape(2048, LANES)
    send = pl.pallas_call(
        middle_kernel,
        out_shape=jax.ShapeDtypeStruct((17 * LANES, LANES), jnp.float32),
        in_specs=in_vmem(3),
        out_specs=pl.BlockSpec(memory_space=pltpu.VMEM),
        scratch_shapes=[pltpu.VMEM((2, count, count), jnp.float32)] * 4,
        compiler_params=params(16),
    )(got, deriv_x, deriv_y)
    got = exchange(send.reshape(LANES, 1, 17 * LANES)).reshape(17 * LANES, LANES)
    potential, energy = pl.pallas_call(
        functools.partial(last_kernel, float(cells)),
        out_shape=(
            jax.ShapeDtypeStruct(density.shape, jnp.float32),
            jax.ShapeDtypeStruct((1, 1), jnp.float32),
        ),
        in_specs=in_vmem(2),
        out_specs=(
            pl.BlockSpec(memory_space=pltpu.VMEM),
            pl.BlockSpec(memory_space=pltpu.SMEM),
        ),
        compiler_params=params(12),
    )(got, deriv_z)
    return potential, energy.reshape(())


def solution(mesh):
    return jax.shard_map(
        functools.partial(body, 256**3),
        mesh=mesh,
        in_specs=(P("gx", "gy", None),),
        out_specs=(P("gx", "gy", None), P()),
        check_vma=False,
    )
```

```python
import functools
import math

import jax
import jax.numpy as jnp
import numpy as np
from jax import lax
from jax.experimental import pallas as pl
from jax.experimental.pallas import tpu as pltpu
from jax.sharding import PartitionSpec as P

AXES = ("gx", "gy")
LANES = 128
VIEW = 8
BLOCK = 32

pbe_kappa = 0.804
pbe_mu = 0.2195149727645171
pbe_beta = 0.06672455060314922
pbe_gamma = 0.031090690869654894
pw_coef = 0.0310907
pw_alpha = 0.2137
pw_first = 7.5957
pw_second = 3.5876
pw_third = 1.6382
pw_fourth = 0.49294

fermi_scale = (3.0 * math.pi**2) ** (1.0 / 3.0)
exch_scale = 0.75 * fermi_scale / math.pi
s_scale = 1.0 / (4.0 * fermi_scale**2)
t_scale = math.pi / (16.0 * fermi_scale)
rs_scale = (3.0 / (4.0 * math.pi)) ** (1.0 / 3.0)
ex_scale = -exch_scale / rs_scale**2
root_slope = -1.0 / (6.0 * math.log(2.0))
root_shift = 0.5 * math.log2(rs_scale)
damping_scale = pbe_mu / pbe_kappa * s_scale / rs_scale**8
tau_scale = pbe_beta / pbe_gamma * t_scale / rs_scale**7
slope_scale = -2.0 * exch_scale * s_scale * pbe_mu / rs_scale**4
weight_scale = 2.0 * pbe_beta * t_scale / rs_scale**4
pw = [2.0 * pw_coef * factor for factor in (pw_first, pw_second, pw_third, pw_fourth)]


def deriv_matrix(count):
    index = np.arange(count)
    signed = np.where(index < count // 2, index, index - count)
    signed = np.where(index == count // 2, 0, signed)
    waves = signed * (2.0 * math.pi / count)
    phase = (index[:, None] * index[None, :] % count) * (2.0 * math.pi / count)
    cosine, sine = np.cos(phase), np.sin(phase)
    return ((cosine * waves) @ sine - (sine * waves) @ cosine) / count


def halves(values):
    high = values.astype(jnp.bfloat16)
    return high, (values - high.astype(jnp.float32)).astype(jnp.bfloat16)


def mul(left, right):
    def dot(first, second):
        return jnp.dot(first, second, preferred_element_type=jnp.float32)

    return dot(left[0], right[0]) + dot(left[1], right[0]) + dot(left[0], right[1])


def pbe(n, g):
    root = jnp.exp2(jnp.log(n) * root_slope + root_shift)
    rs = root * root
    rs2 = rs * rs
    rs4 = rs2 * rs2
    scaled = g * rs4
    damping = 1.0 + damping_scale * (scaled * rs4)
    tau = tau_scale * (scaled * (rs2 * rs))
    part = n * rs2
    series = root * (pw[0] + root * (pw[1] + root * (pw[2] + root * pw[3])))
    third = root * (
        pw[0] / 6 + root * (pw[1] / 3 + root * (pw[2] / 2 + root * (pw[3] / 1.5)))
    )
    outer = 1.0 + series
    product = series * outer
    inverse = 1.0 / (product * damping)
    damp = product * inverse
    fraction = damping * inverse
    logarithm = jnp.log(1.0 + outer * fraction)
    curved = (-2.0 * pw_coef * pw_alpha) * rs
    front = curved - 2.0 * pw_coef
    ec = front * logarithm
    n_dec = front * (third * fraction) - (curved * (1.0 / 3.0)) * logarithm
    grown = jnp.exp2(ec * (-1.0 / (pbe_gamma * math.log(2.0))))
    m = grown - 1.0
    m2 = m * m
    cross = tau * m
    tau2 = tau * tau
    near = m + tau
    base = m2 + cross + tau2
    top = base + cross * near
    both = 1.0 / (base * top)
    rest = ec + pbe_gamma * jnp.log(top * (top * both))
    damp2 = damp * damp
    energy = part * ((1.0 + pbe_kappa) * ex_scale - (pbe_kappa * ex_scale) * damp) + rest
    weight = (near + tau) * (m2 * m)
    twice = rs4 * (slope_scale * damp2 + (weight_scale * weight) * both)
    n_dh = (tau * both) * (
        (-7.0 / 3.0 * pbe_gamma) * weight - tau2 * ((near + m) * (grown * n_dec))
    )
    d_dens = (
        part
        * (
            (4.0 / 3.0) * (1.0 + pbe_kappa) * ex_scale
            + damp * ((-4.0 * pbe_kappa * ex_scale) + (8.0 / 3.0 * pbe_kappa * ex_scale) * damp)
        )
        + (rest + n_dec)
        + n_dh
    )
    return n * energy, d_dens, twice


def mix(parts, odd, upper):
    pairs = [jnp.where(odd, parts[(1 - t) % 4], parts[-t % 4]) for t in range(4)]
    return [jnp.where(upper, pairs[(t + 2) % 4], pairs[t]) for t in range(4)]


def swap_rows(first, second, below):
    return (
        jnp.where(below, pltpu.roll(second, 4, 0), first),
        jnp.where(below, second, pltpu.roll(first, 4, 0)),
    )


def masks():
    lane = lax.broadcasted_iota(jnp.int32, (VIEW, LANES), 1)
    row = lax.broadcasted_iota(jnp.int32, (VIEW, LANES), 0)
    return (lane & 32) != 0, (lane & 64) != 0, (row & 4) != 0


def turn():
    return lax.rem(lax.axis_index("gy"), 4)


def first_kernel(density_hbm, deriv_hbm, send_ref, density_ref, deriv_ref, wide_ref, sems):
    copies = [
        pltpu.make_async_copy(density_hbm, density_ref, sems.at[0]),
        pltpu.make_async_copy(deriv_hbm, deriv_ref, sems.at[1]),
    ]
    for copy in copies:
        copy.start()
    back = 4 - turn()
    copies[0].wait()
    lines = jnp.concatenate(
        [density_ref[4 * (place // 4) + lax.rem(place % 4 + back, 4)] for place in range(16)]
    )
    turned = lines.T
    copies[1].wait()
    slopes = mul((deriv_ref[0], deriv_ref[1]), halves(turned))
    rows = 2 * VIEW
    for field, values in enumerate((turned, slopes)):
        for plane in range(2):
            for part in range(4):
                row = VIEW * field + 4 * plane + part
                wide_ref[pl.ds(row, LANES, stride=rows + 1), :] = values[
                    LANES * plane : LANES * (plane + 1), LANES * part : LANES * (part + 1)
                ]
    for other in range(LANES):
        start = (rows + 1) * other
        send_ref[rows * other : rows * (other + 1), :] = wide_ref[start : start + rows, :]


def middle_kernel(
    got_ref, deriv_x_ref, deriv_y_ref, send_ref, dens_ref, grad_z_ref, grad_x_ref, grad_y_ref
):
    rows = 2 * VIEW
    odd, upper, below = masks()

    def receive(a, field, ref):
        for half in range(2):
            parts = []
            for quarter in range(4):
                start = a * (8 * rows) + ((half * 4 + quarter) * rows + VIEW * field)
                parts.append(got_ref[start : start + VIEW, :])
            parts = [
                pltpu.roll(part, LANES - 32 * t, 1) if t else part
                for t, part in enumerate(mix(parts, odd, upper))
            ]
            for pair in range(2):
                planes = swap_rows(parts[2 * pair], parts[2 * pair + 1], below)
                for plane in range(2):
                    start = a * 16 + pair * VIEW
                    ref[
                        plane, start : start + VIEW, LANES * half : LANES * (half + 1)
                    ] = planes[plane]

    def give(a, field, ref):
        for half in range(2):
            parts = []
            for pair in range(2):
                start = a * 16 + pair * VIEW
                planes = [
                    ref[plane, start : start + VIEW, LANES * half : LANES * (half + 1)]
                    for plane in range(2)
                ]
                parts.extend(swap_rows(*planes, below))
            parts = [pltpu.roll(part, 32 * t, 1) if t else part for t, part in enumerate(parts)]
            for quarter, part in enumerate(mix(parts, odd, upper)):
                start = ((a * 2 + half) * 4 + quarter) * (rows + 1) + VIEW * field
                send_ref[start : start + VIEW, :] = part

    def slopes(plane):
        dens = halves(dens_ref[plane])
        grad_x_ref[plane] = mul((deriv_x_ref[0], deriv_x_ref[1]), dens)
        grad_y_ref[plane] = mul(dens, (deriv_y_ref[0], deriv_y_ref[1]))

    def subtract(plane):
        dens_ref[plane] = (
            dens_ref[plane]
            - mul((deriv_x_ref[0], deriv_x_ref[1]), halves(grad_x_ref[plane]))
            - mul(halves(grad_y_ref[plane]), (deriv_y_ref[0], deriv_y_ref[1]))
        )

    def evaluate(plane, total):
        for start in range(0, 256, BLOCK):
            block = plane, slice(start, start + BLOCK)
            n = dens_ref[block]
            gx, gy, gz = grad_x_ref[block], grad_y_ref[block], grad_z_ref[block]
            f, d_dens, twice = pbe(n, gx * gx + gy * gy + gz * gz)
            grad_x_ref[block] = twice * gx
            grad_y_ref[block] = twice * gy
            grad_z_ref[block] = twice * gz
            dens_ref[block] = d_dens
            total = total + f
        return total

    for a in range(16):
        receive(a, 0, dens_ref)
    slopes(0)
    for a in range(16):
        receive(a, 1, grad_z_ref)
    total = evaluate(0, jnp.zeros((BLOCK, 256), jnp.float32))
    slopes(1)
    subtract(0)
    total = evaluate(1, total)
    subtract(1)
    for a in range(16):
        give(a, 1, grad_z_ref)
    for a in range(16):
        give(a, 0, dens_ref)
    summed = jnp.sum(total[:, :LANES] + total[:, LANES:], axis=0, keepdims=True)
    send_ref[pl.ds(rows, LANES, stride=rows + 1), :] = jnp.broadcast_to(summed, (LANES, LANES))


def last_kernel(cells, got_ref, deriv_ref, potential_ref, energy_ref):
    rows = 2 * VIEW + 1
    back = 4 - turn()

    def gather(field):
        return jnp.concatenate(
            [
                jnp.concatenate(
                    [
                        got_ref[pl.ds(VIEW * field + 4 * plane + part, LANES, stride=rows), :]
                        for part in range(4)
                    ],
                    axis=1,
                )
                for plane in range(2)
            ],
            axis=0,
        )

    turned = gather(0) - mul((deriv_ref[0], deriv_ref[1]), halves(gather(1)))
    lines = turned.T
    for place in range(16):
        potential_ref[4 * (place // 4) + lax.rem(place % 4 + back, 4)] = lines[
            32 * place : 32 * (place + 1)
        ]
    energy_ref[0, 0] = jnp.sum(got_ref[pl.ds(rows - 1, LANES, stride=rows), :]) / cells


def params(megabytes):
    return pltpu.CompilerParams(vmem_limit_bytes=megabytes << 20)


def in_vmem(count):
    return [pl.BlockSpec(memory_space=pltpu.VMEM)] * count


def far(values):
    return pltpu.with_memory_space_constraint(values, pltpu.HBM)


def exchange(values):
    return lax.all_to_all(values, AXES, split_axis=0, concat_axis=0, tiled=True)


def pair(matrix):
    high = matrix.astype(jnp.bfloat16)
    low = (matrix - high.astype(np.float64)).astype(jnp.bfloat16)
    return jnp.asarray(np.stack([high, low]))


def body(cells, density):
    count = density.shape[-1]
    deriv = deriv_matrix(count)
    row = np.arange(count)
    cell = 16 * (row // 16) + 4 * (row % 4) + (row // 4) % 4
    deriv_z = pair(deriv)
    deriv_y = pair(deriv.T)
    deriv_x = pair(deriv[cell[:, None], cell[None, :]])

    send = pl.pallas_call(
        first_kernel,
        out_shape=jax.ShapeDtypeStruct((2048, LANES), jnp.float32),
        in_specs=[pl.BlockSpec(memory_space=pltpu.HBM)] * 2,
        out_specs=pl.BlockSpec(memory_space=pltpu.VMEM),
        scratch_shapes=[
            pltpu.VMEM(density.shape, jnp.float32),
            pltpu.VMEM((2, count, count), jnp.bfloat16),
            pltpu.VMEM((17 * LANES, LANES), jnp.float32),
            pltpu.SemaphoreType.DMA((2,)),
        ],
        compiler_params=params(12),
    )(far(density), far(deriv_z))
    got = exchange(send.reshape(LANES, 16, LANES)).reshape(2048, LANES)
    send = pl.pallas_call(
        middle_kernel,
        out_shape=jax.ShapeDtypeStruct((17 * LANES, LANES), jnp.float32),
        in_specs=in_vmem(3),
        out_specs=pl.BlockSpec(memory_space=pltpu.VMEM),
        scratch_shapes=[pltpu.VMEM((2, count, count), jnp.float32)] * 4,
        compiler_params=params(16),
    )(got, deriv_x, deriv_y)
    got = exchange(send.reshape(LANES, 1, 17 * LANES)).reshape(17 * LANES, LANES)
    potential, energy = pl.pallas_call(
        functools.partial(last_kernel, float(cells)),
        out_shape=(
            jax.ShapeDtypeStruct(density.shape, jnp.float32),
            jax.ShapeDtypeStruct((1, 1), jnp.float32),
        ),
        in_specs=in_vmem(2),
        out_specs=(
            pl.BlockSpec(memory_space=pltpu.VMEM),
            pl.BlockSpec(memory_space=pltpu.SMEM),
        ),
        compiler_params=params(12),
    )(got, deriv_z)
    return potential, energy.reshape(())


def solution(mesh):
    return jax.shard_map(
        functools.partial(body, 256**3),
        mesh=mesh,
        in_specs=(P("gx", "gy", None),),
        out_specs=(P("gx", "gy", None), P()),
        check_vma=False,
    )
```

```python
import functools
import math

import jax
import jax.numpy as jnp
import numpy as np
from jax import lax
from jax.experimental import pallas as pl
from jax.experimental.pallas import tpu as pltpu
from jax.sharding import PartitionSpec as P

AXES = ("gx", "gy")
LANES = 128
VIEW = 8
BLOCK = 32

pbe_kappa = 0.804
pbe_mu = 0.2195149727645171
pbe_beta = 0.06672455060314922
pbe_gamma = 0.031090690869654894
pw_coef = 0.0310907
pw_alpha = 0.2137
pw_first = 7.5957
pw_second = 3.5876
pw_third = 1.6382
pw_fourth = 0.49294

fermi_scale = (3.0 * math.pi**2) ** (1.0 / 3.0)
exch_scale = 0.75 * fermi_scale / math.pi
s_scale = 1.0 / (4.0 * fermi_scale**2)
t_scale = math.pi / (16.0 * fermi_scale)
rs_scale = (3.0 / (4.0 * math.pi)) ** (1.0 / 3.0)
ex_scale = -exch_scale / rs_scale**2
root_slope = -1.0 / (6.0 * math.log(2.0))
root_shift = 0.5 * math.log2(rs_scale)
damping_scale = pbe_mu / pbe_kappa * s_scale / rs_scale**8
tau_scale = pbe_beta / pbe_gamma * t_scale / rs_scale**7
slope_scale = -2.0 * exch_scale * s_scale * pbe_mu / rs_scale**4
weight_scale = 2.0 * pbe_beta * t_scale / rs_scale**4
pw = [2.0 * pw_coef * factor for factor in (pw_first, pw_second, pw_third, pw_fourth)]


def deriv_matrix(count):
    index = np.arange(count)
    signed = np.where(index < count // 2, index, index - count)
    signed = np.where(index == count // 2, 0, signed)
    waves = signed * (2.0 * math.pi / count)
    phase = (index[:, None] * index[None, :] % count) * (2.0 * math.pi / count)
    cosine, sine = np.cos(phase), np.sin(phase)
    return ((cosine * waves) @ sine - (sine * waves) @ cosine) / count


def halves(values):
    high = values.astype(jnp.bfloat16)
    return high, (values - high.astype(jnp.float32)).astype(jnp.bfloat16)


def mul(left, right, axis=0):
    def dot(first, second):
        return lax.dot_general(
            first, second, (((1,), (axis,)), ((), ())), preferred_element_type=jnp.float32
        )

    return dot(left[0], right[0]) + dot(left[1], right[0]) + dot(left[0], right[1])


def pbe(n, g):
    root = jnp.exp2(jnp.log(n) * root_slope + root_shift)
    rs = root * root
    rs2 = rs * rs
    rs4 = rs2 * rs2
    scaled = g * rs4
    damping = 1.0 + damping_scale * (scaled * rs4)
    tau = tau_scale * (scaled * (rs2 * rs))
    part = n * rs2
    series = root * (pw[0] + root * (pw[1] + root * (pw[2] + root * pw[3])))
    third = root * (
        pw[0] / 6 + root * (pw[1] / 3 + root * (pw[2] / 2 + root * (pw[3] / 1.5)))
    )
    damp = 1.0 / damping
    flipped = 1.0 / series
    fraction = flipped * (1.0 / (1.0 + series))
    logarithm = jnp.log(1.0 + flipped)
    curved = (-2.0 * pw_coef * pw_alpha) * rs
    front = curved - 2.0 * pw_coef
    ec = front * logarithm
    n_dec = front * (third * fraction) - (curved * (1.0 / 3.0)) * logarithm
    grown = jnp.exp2(ec * (-1.0 / (pbe_gamma * math.log(2.0))))
    m = grown - 1.0
    m2 = m * m
    cross = tau * m
    tau2 = tau * tau
    near = m + tau
    base = m2 + cross + tau2
    top = base + cross * near
    lower = 1.0 / base
    both = lower * (1.0 / top)
    rest = ec + pbe_gamma * jnp.log(top * lower)
    damp2 = damp * damp
    energy = part * ((1.0 + pbe_kappa) * ex_scale - (pbe_kappa * ex_scale) * damp) + rest
    weight = (near + tau) * (m2 * m)
    twice = rs4 * (slope_scale * damp2 + (weight_scale * weight) * both)
    n_dh = (tau * both) * (
        (-7.0 / 3.0 * pbe_gamma) * weight - tau2 * ((near + m) * (grown * n_dec))
    )
    d_dens = (
        part
        * (
            (4.0 / 3.0) * (1.0 + pbe_kappa) * ex_scale
            + damp * ((-4.0 * pbe_kappa * ex_scale) + (8.0 / 3.0 * pbe_kappa * ex_scale) * damp)
        )
        + (rest + n_dec)
        + n_dh
    )
    return n * energy, d_dens, twice


def mix(parts, odd, upper):
    pairs = [jnp.where(odd, parts[(1 - t) % 4], parts[-t % 4]) for t in range(4)]
    return [jnp.where(upper, pairs[(t + 2) % 4], pairs[t]) for t in range(4)]


def swap_rows(first, second, below):
    return (
        jnp.where(below, pltpu.roll(second, 4, 0), first),
        jnp.where(below, second, pltpu.roll(first, 4, 0)),
    )


def masks():
    lane = lax.broadcasted_iota(jnp.int32, (VIEW, LANES), 1)
    row = lax.broadcasted_iota(jnp.int32, (VIEW, LANES), 0)
    return (lane & 32) != 0, (lane & 64) != 0, (row & 4) != 0


def turn():
    return lax.rem(lax.axis_index("gy"), 4)


def first_kernel(density_hbm, deriv_hbm, send_ref, density_ref, deriv_ref, wide_ref, sems):
    copies = [
        pltpu.make_async_copy(density_hbm, density_ref, sems.at[0]),
        pltpu.make_async_copy(deriv_hbm, deriv_ref, sems.at[1]),
    ]
    for copy in copies:
        copy.start()
    back = 4 - turn()
    for copy in copies:
        copy.wait()
    lines = jnp.concatenate(
        [density_ref[4 * (place // 4) + lax.rem(place % 4 + back, 4)] for place in range(16)]
    )
    turned = lines.T
    slopes = mul((deriv_ref[0], deriv_ref[1]), halves(lines), 1)
    rows = 2 * VIEW
    for field, values in enumerate((turned, slopes)):
        for plane in range(2):
            for part in range(4):
                row = VIEW * field + 4 * plane + part
                wide_ref[pl.ds(row, LANES, stride=rows + 1), :] = values[
                    LANES * plane : LANES * (plane + 1), LANES * part : LANES * (part + 1)
                ]
    for other in range(LANES):
        start = (rows + 1) * other
        send_ref[rows * other : rows * (other + 1), :] = wide_ref[start : start + rows, :]


def middle_kernel(
    got_ref, deriv_x_ref, deriv_y_ref, send_ref, dens_ref, grad_z_ref, grad_x_ref, grad_y_ref
):
    rows = 2 * VIEW
    odd, upper, below = masks()

    def receive(a, field, ref):
        for half in range(2):
            parts = []
            for quarter in range(4):
                start = a * (8 * rows) + ((half * 4 + quarter) * rows + VIEW * field)
                parts.append(got_ref[start : start + VIEW, :])
            parts = [
                pltpu.roll(part, LANES - 32 * t, 1) if t else part
                for t, part in enumerate(mix(parts, odd, upper))
            ]
            for pair in range(2):
                planes = swap_rows(parts[2 * pair], parts[2 * pair + 1], below)
                for plane in range(2):
                    start = a * 16 + pair * VIEW
                    ref[
                        plane, start : start + VIEW, LANES * half : LANES * (half + 1)
                    ] = planes[plane]

    def give(a, field, ref):
        for half in range(2):
            parts = []
            for pair in range(2):
                start = a * 16 + pair * VIEW
                planes = [
                    ref[plane, start : start + VIEW, LANES * half : LANES * (half + 1)]
                    for plane in range(2)
                ]
                parts.extend(swap_rows(*planes, below))
            parts = [pltpu.roll(part, 32 * t, 1) if t else part for t, part in enumerate(parts)]
            for quarter, part in enumerate(mix(parts, odd, upper)):
                start = ((a * 2 + half) * 4 + quarter) * (rows + 1) + VIEW * field
                send_ref[start : start + VIEW, :] = part

    def slopes(plane):
        dens = halves(dens_ref[plane])
        grad_x_ref[plane] = mul((deriv_x_ref[0], deriv_x_ref[1]), dens)
        grad_y_ref[plane] = mul(dens, (deriv_y_ref[0], deriv_y_ref[1]))

    def subtract(plane):
        dens_ref[plane] = (
            dens_ref[plane]
            - mul((deriv_x_ref[0], deriv_x_ref[1]), halves(grad_x_ref[plane]))
            - mul(halves(grad_y_ref[plane]), (deriv_y_ref[0], deriv_y_ref[1]))
        )

    def evaluate(plane, total):
        for start in range(0, 256, BLOCK):
            block = plane, slice(start, start + BLOCK)
            n = dens_ref[block]
            gx, gy, gz = grad_x_ref[block], grad_y_ref[block], grad_z_ref[block]
            f, d_dens, twice = pbe(n, gx * gx + gy * gy + gz * gz)
            grad_x_ref[block] = twice * gx
            grad_y_ref[block] = twice * gy
            grad_z_ref[block] = twice * gz
            dens_ref[block] = d_dens
            total = total + f
        return total

    for a in range(16):
        receive(a, 0, dens_ref)
    slopes(0)
    for a in range(16):
        receive(a, 1, grad_z_ref)
    total = evaluate(0, jnp.zeros((BLOCK, 256), jnp.float32))
    slopes(1)
    subtract(0)
    total = evaluate(1, total)
    subtract(1)
    for a in range(16):
        give(a, 1, grad_z_ref)
    for a in range(16):
        give(a, 0, dens_ref)
    summed = jnp.sum(total[:, :LANES] + total[:, LANES:], axis=0, keepdims=True)
    send_ref[pl.ds(rows, LANES, stride=rows + 1), :] = jnp.broadcast_to(summed, (LANES, LANES))


def last_kernel(cells, got_ref, deriv_ref, potential_ref, energy_ref):
    rows = 2 * VIEW + 1
    back = 4 - turn()

    def gather(field):
        return jnp.concatenate(
            [
                jnp.concatenate(
                    [
                        got_ref[pl.ds(VIEW * field + 4 * plane + part, LANES, stride=rows), :]
                        for part in range(4)
                    ],
                    axis=1,
                )
                for plane in range(2)
            ],
            axis=0,
        )

    turned = gather(0) - mul((deriv_ref[0], deriv_ref[1]), halves(gather(1)))
    lines = turned.T
    for place in range(16):
        potential_ref[4 * (place // 4) + lax.rem(place % 4 + back, 4)] = lines[
            32 * place : 32 * (place + 1)
        ]
    energy_ref[0, 0] = jnp.sum(got_ref[pl.ds(rows - 1, LANES, stride=rows), :]) / cells


def params(megabytes):
    return pltpu.CompilerParams(vmem_limit_bytes=megabytes << 20)


def in_vmem(count):
    return [pl.BlockSpec(memory_space=pltpu.VMEM)] * count


def far(values):
    return pltpu.with_memory_space_constraint(values, pltpu.HBM)


def exchange(values):
    return lax.all_to_all(values, AXES, split_axis=0, concat_axis=0, tiled=True)


def pair(matrix):
    high = matrix.astype(jnp.bfloat16)
    low = (matrix - high.astype(np.float64)).astype(jnp.bfloat16)
    return jnp.asarray(np.stack([high, low]))


def body(cells, density):
    count = density.shape[-1]
    deriv = deriv_matrix(count)
    row = np.arange(count)
    cell = 16 * (row // 16) + 4 * (row % 4) + (row // 4) % 4
    deriv_z = pair(deriv)
    deriv_y = pair(deriv.T)
    deriv_x = pair(deriv[cell[:, None], cell[None, :]])

    send = pl.pallas_call(
        first_kernel,
        out_shape=jax.ShapeDtypeStruct((2048, LANES), jnp.float32),
        in_specs=[pl.BlockSpec(memory_space=pltpu.HBM)] * 2,
        out_specs=pl.BlockSpec(memory_space=pltpu.VMEM),
        scratch_shapes=[
            pltpu.VMEM(density.shape, jnp.float32),
            pltpu.VMEM((2, count, count), jnp.bfloat16),
            pltpu.VMEM((17 * LANES, LANES), jnp.float32),
            pltpu.SemaphoreType.DMA((2,)),
        ],
        compiler_params=params(12),
    )(far(density), far(deriv_z))
    got = exchange(send.reshape(LANES, 16, LANES)).reshape(2048, LANES)
    send = pl.pallas_call(
        middle_kernel,
        out_shape=jax.ShapeDtypeStruct((17 * LANES, LANES), jnp.float32),
        in_specs=in_vmem(3),
        out_specs=pl.BlockSpec(memory_space=pltpu.VMEM),
        scratch_shapes=[pltpu.VMEM((2, count, count), jnp.float32)] * 4,
        compiler_params=params(16),
    )(got, deriv_x, deriv_y)
    got = exchange(send.reshape(LANES, 1, 17 * LANES)).reshape(17 * LANES, LANES)
    potential, energy = pl.pallas_call(
        functools.partial(last_kernel, float(cells)),
        out_shape=(
            jax.ShapeDtypeStruct(density.shape, jnp.float32),
            jax.ShapeDtypeStruct((1, 1), jnp.float32),
        ),
        in_specs=in_vmem(2),
        out_specs=(
            pl.BlockSpec(memory_space=pltpu.VMEM),
            pl.BlockSpec(memory_space=pltpu.SMEM),
        ),
        compiler_params=params(12),
    )(got, deriv_z)
    return potential, energy.reshape(())


def solution(mesh):
    return jax.shard_map(
        functools.partial(body, 256**3),
        mesh=mesh,
        in_specs=(P("gx", "gy", None),),
        out_specs=(P("gx", "gy", None), P()),
        check_vma=False,
    )
```

```python
import functools
import math

import jax
import jax.numpy as jnp
import numpy as np
from jax import lax
from jax.experimental import pallas as pl
from jax.experimental.pallas import tpu as pltpu
from jax.sharding import Mesh
from jax.sharding import PartitionSpec as P

GX = ("z1", "z0", "yh", "core")
GY = ("yl", "x1", "x0")
ORDER = ("core", "yh", "yl", "x1", "x0", "z1", "z0")
LANES = 128
VIEW = 8
BLOCK = 32

pbe_kappa = 0.804
pbe_mu = 0.2195149727645171
pbe_beta = 0.06672455060314922
pbe_gamma = 0.031090690869654894
pw_coef = 0.0310907
pw_alpha = 0.2137
pw_first = 7.5957
pw_second = 3.5876
pw_third = 1.6382
pw_fourth = 0.49294

fermi_scale = (3.0 * math.pi**2) ** (1.0 / 3.0)
exch_scale = 0.75 * fermi_scale / math.pi
s_scale = 1.0 / (4.0 * fermi_scale**2)
t_scale = math.pi / (16.0 * fermi_scale)
rs_scale = (3.0 / (4.0 * math.pi)) ** (1.0 / 3.0)
ex_scale = -exch_scale / rs_scale**2
root_slope = -1.0 / (6.0 * math.log(2.0))
root_shift = 0.5 * math.log2(rs_scale)
damping_scale = pbe_mu / pbe_kappa * s_scale / rs_scale**8
tau_scale = pbe_beta / pbe_gamma * t_scale / rs_scale**7
slope_scale = -2.0 * exch_scale * s_scale * pbe_mu / rs_scale**4
weight_scale = 2.0 * pbe_beta * t_scale / rs_scale**4
pw = [2.0 * pw_coef * factor for factor in (pw_first, pw_second, pw_third, pw_fourth)]


def deriv_matrix(count):
    index = np.arange(count)
    signed = np.where(index < count // 2, index, index - count)
    signed = np.where(index == count // 2, 0, signed)
    waves = signed * (2.0 * math.pi / count)
    phase = (index[:, None] * index[None, :] % count) * (2.0 * math.pi / count)
    cosine, sine = np.cos(phase), np.sin(phase)
    return ((cosine * waves) @ sine - (sine * waves) @ cosine) / count


def halves(values):
    high = values.astype(jnp.bfloat16)
    return high, (values - high.astype(jnp.float32)).astype(jnp.bfloat16)


def mul(left, right, axis=0):
    def dot(first, second):
        return lax.dot_general(
            first, second, (((1,), (axis,)), ((), ())), preferred_element_type=jnp.float32
        )

    return dot(left[0], right[0]) + dot(left[1], right[0]) + dot(left[0], right[1])


def pbe(n, g):
    root = jnp.exp2(jnp.log(n) * root_slope + root_shift)
    rs = root * root
    rs2 = rs * rs
    rs4 = rs2 * rs2
    scaled = g * rs4
    damping = 1.0 + damping_scale * (scaled * rs4)
    tau = tau_scale * (scaled * (rs2 * rs))
    part = n * rs2
    series = root * (pw[0] + root * (pw[1] + root * (pw[2] + root * pw[3])))
    third = root * (
        pw[0] / 6 + root * (pw[1] / 3 + root * (pw[2] / 2 + root * (pw[3] / 1.5)))
    )
    damp = 1.0 / damping
    flipped = 1.0 / series
    fraction = flipped * (1.0 / (1.0 + series))
    logarithm = jnp.log(1.0 + flipped)
    curved = (-2.0 * pw_coef * pw_alpha) * rs
    front = curved - 2.0 * pw_coef
    ec = front * logarithm
    n_dec = front * (third * fraction) - (curved * (1.0 / 3.0)) * logarithm
    grown = jnp.exp2(ec * (-1.0 / (pbe_gamma * math.log(2.0))))
    m = grown - 1.0
    m2 = m * m
    cross = tau * m
    tau2 = tau * tau
    near = m + tau
    base = m2 + cross + tau2
    top = base + cross * near
    lower = 1.0 / base
    both = lower * (1.0 / top)
    rest = ec + pbe_gamma * jnp.log(top * lower)
    damp2 = damp * damp
    energy = part * ((1.0 + pbe_kappa) * ex_scale - (pbe_kappa * ex_scale) * damp) + rest
    weight = (near + tau) * (m2 * m)
    twice = rs4 * (slope_scale * damp2 + (weight_scale * weight) * both)
    n_dh = (tau * both) * (
        (-7.0 / 3.0 * pbe_gamma) * weight - tau2 * ((near + m) * (grown * n_dec))
    )
    d_dens = (
        part
        * (
            (4.0 / 3.0) * (1.0 + pbe_kappa) * ex_scale
            + damp * ((-4.0 * pbe_kappa * ex_scale) + (8.0 / 3.0 * pbe_kappa * ex_scale) * damp)
        )
        + (rest + n_dec)
        + n_dh
    )
    return n * energy, d_dens, twice


def mix(parts, odd, upper):
    pairs = [jnp.where(odd, parts[(1 - t) % 4], parts[-t % 4]) for t in range(4)]
    return [jnp.where(upper, pairs[(t + 2) % 4], pairs[t]) for t in range(4)]


def place(a, b):
    at = {axis: a >> (3 - i) & 1 for i, axis in enumerate(GX)}
    at |= {axis: b >> (2 - i) & 1 for i, axis in enumerate(GY)}
    return functools.reduce(lambda index, axis: 2 * index + at[axis], ORDER, 0)


def masks():
    lane = lax.broadcasted_iota(jnp.int32, (VIEW, LANES), 1)
    row = lax.broadcasted_iota(jnp.int32, (VIEW, LANES), 0)
    return (lane & 32) != 0, (lane & 64) != 0, (row & 4) != 0


def turn():
    return 2 * lax.axis_index("x1") + lax.axis_index("x0")


def first_kernel(density_hbm, deriv_hbm, send_ref, density_ref, deriv_ref, wide_ref, sems):
    copies = [
        pltpu.make_async_copy(density_hbm, density_ref, sems.at[0]),
        pltpu.make_async_copy(deriv_hbm, deriv_ref, sems.at[1]),
    ]
    for copy in copies:
        copy.start()
    back = 4 - turn()
    for copy in copies:
        copy.wait()
    lines = jnp.concatenate(
        [density_ref[4 * (place // 4) + lax.rem(place % 4 + back, 4)] for place in range(16)]
    )
    turned = lines.T
    slopes = mul((deriv_ref[0], deriv_ref[1]), halves(lines), 1)
    rows = 2 * VIEW
    for field, values in enumerate((turned, slopes)):
        for plane in range(2):
            for part in range(4):
                row = VIEW * field + 4 * plane + part
                wide_ref[pl.ds(row, LANES, stride=rows + 1), :] = values[
                    LANES * plane : LANES * (plane + 1), LANES * part : LANES * (part + 1)
                ]
    for other in range(LANES):
        start = (rows + 1) * other
        send_ref[rows * other : rows * (other + 1), :] = wide_ref[start : start + rows, :]


def middle_kernel(
    got_ref, deriv_x_ref, deriv_y_ref, send_ref, dens_ref, grad_z_ref, grad_x_ref, grad_y_ref
):
    rows = 2 * VIEW
    odd, upper, below = masks()

    def receive(pair, field, ref):
        for half in range(2):
            for plane in range(2):
                parts = []
                for quarter in range(4):
                    block = 4 * half + quarter
                    shift = VIEW * field + 4 * plane
                    start = place(2 * pair, block) * rows + shift
                    later = place(2 * pair + 1, block) * rows + shift - 4
                    parts.append(
                        jnp.where(
                            below, got_ref[later : later + VIEW, :], got_ref[start : start + VIEW, :]
                        )
                    )
                for t, part in enumerate(mix(parts, odd, upper)):
                    start = (pair * 4 + t) * VIEW
                    ref[plane, start : start + VIEW, LANES * half : LANES * (half + 1)] = (
                        pltpu.roll(part, LANES - 32 * t, 1) if t else part
                    )

    def give(pair, field, ref):
        for half in range(2):
            for plane in range(2):
                parts = []
                for t in range(4):
                    start = (pair * 4 + t) * VIEW
                    part = ref[plane, start : start + VIEW, LANES * half : LANES * (half + 1)]
                    parts.append(pltpu.roll(part, 32 * t, 1) if t else part)
                for quarter, part in enumerate(mix(parts, odd, upper)):
                    block = 4 * half + quarter
                    shift = VIEW * field + 4 * plane
                    start = place(2 * pair, block) * (rows + 1) + shift
                    later = place(2 * pair + 1, block) * (rows + 1) + shift
                    send_ref[start : start + 4, :] = part[:4]
                    send_ref[later : later + 4, :] = part[4:]

    def slopes(plane):
        dens = halves(dens_ref[plane])
        grad_x_ref[plane] = mul((deriv_x_ref[0], deriv_x_ref[1]), dens)
        grad_y_ref[plane] = mul(dens, (deriv_y_ref[0], deriv_y_ref[1]))

    def subtract(plane):
        dens_ref[plane] = (
            dens_ref[plane]
            - mul((deriv_x_ref[0], deriv_x_ref[1]), halves(grad_x_ref[plane]))
            - mul(halves(grad_y_ref[plane]), (deriv_y_ref[0], deriv_y_ref[1]))
        )

    def evaluate(plane, total):
        for start in range(0, 256, BLOCK):
            block = plane, slice(start, start + BLOCK)
            n = dens_ref[block]
            gx, gy, gz = grad_x_ref[block], grad_y_ref[block], grad_z_ref[block]
            f, d_dens, twice = pbe(n, gx * gx + gy * gy + gz * gz)
            grad_x_ref[block] = twice * gx
            grad_y_ref[block] = twice * gy
            grad_z_ref[block] = twice * gz
            dens_ref[block] = d_dens
            total = total + f
        return total

    for pair in range(8):
        receive(pair, 0, dens_ref)
    slopes(0)
    for pair in range(8):
        receive(pair, 1, grad_z_ref)
    total = evaluate(0, jnp.zeros((BLOCK, 256), jnp.float32))
    slopes(1)
    subtract(0)
    total = evaluate(1, total)
    subtract(1)
    for pair in range(8):
        give(pair, 1, grad_z_ref)
    for pair in range(8):
        give(pair, 0, dens_ref)
    summed = jnp.sum(total[:, :LANES] + total[:, LANES:], axis=0, keepdims=True)
    send_ref[pl.ds(rows, LANES, stride=rows + 1), :] = jnp.broadcast_to(summed, (LANES, LANES))


def last_kernel(cells, got_ref, deriv_ref, potential_ref, energy_ref):
    rows = 2 * VIEW + 1
    back = 4 - turn()

    def gather(field):
        return jnp.concatenate(
            [
                jnp.concatenate(
                    [
                        got_ref[pl.ds(VIEW * field + 4 * plane + part, LANES, stride=rows), :]
                        for part in range(4)
                    ],
                    axis=1,
                )
                for plane in range(2)
            ],
            axis=0,
        )

    turned = gather(0) - mul((deriv_ref[0], deriv_ref[1]), halves(gather(1)))
    lines = turned.T
    for place in range(16):
        potential_ref[4 * (place // 4) + lax.rem(place % 4 + back, 4)] = lines[
            32 * place : 32 * (place + 1)
        ]
    energy_ref[0, 0] = jnp.sum(got_ref[pl.ds(rows - 1, LANES, stride=rows), :]) / cells


def params(megabytes):
    return pltpu.CompilerParams(vmem_limit_bytes=megabytes << 20)


def in_vmem(count):
    return [pl.BlockSpec(memory_space=pltpu.VMEM)] * count


def far(values):
    return pltpu.with_memory_space_constraint(values, pltpu.HBM)


def exchange(values):
    return lax.all_to_all(values, ORDER, split_axis=0, concat_axis=0, tiled=True)


def pair(matrix):
    high = matrix.astype(jnp.bfloat16)
    low = (matrix - high.astype(np.float64)).astype(jnp.bfloat16)
    return jnp.asarray(np.stack([high, low]))


def body(cells, density):
    count = density.shape[-1]
    deriv = deriv_matrix(count)
    row = np.arange(count)
    cell = 16 * (2 * (row // 32) + (row // 4) % 2) + 4 * (row % 4) + (row // 8) % 4
    deriv_z = pair(deriv)
    deriv_y = pair(deriv.T)
    deriv_x = pair(deriv[cell[:, None], cell[None, :]])

    send = pl.pallas_call(
        first_kernel,
        out_shape=jax.ShapeDtypeStruct((2048, LANES), jnp.float32),
        in_specs=[pl.BlockSpec(memory_space=pltpu.HBM)] * 2,
        out_specs=pl.BlockSpec(memory_space=pltpu.VMEM),
        scratch_shapes=[
            pltpu.VMEM(density.shape, jnp.float32),
            pltpu.VMEM((2, count, count), jnp.bfloat16),
            pltpu.VMEM((17 * LANES, LANES), jnp.float32),
            pltpu.SemaphoreType.DMA((2,)),
        ],
        compiler_params=params(12),
    )(far(density), far(deriv_z))
    got = exchange(send.reshape(LANES, 16, LANES)).reshape(2048, LANES)
    send = pl.pallas_call(
        middle_kernel,
        out_shape=jax.ShapeDtypeStruct((17 * LANES, LANES), jnp.float32),
        in_specs=in_vmem(3),
        out_specs=pl.BlockSpec(memory_space=pltpu.VMEM),
        scratch_shapes=[pltpu.VMEM((2, count, count), jnp.float32)] * 4,
        compiler_params=params(16),
    )(got, deriv_x, deriv_y)
    got = exchange(send.reshape(LANES, 1, 17 * LANES)).reshape(17 * LANES, LANES)
    potential, energy = pl.pallas_call(
        functools.partial(last_kernel, float(cells)),
        out_shape=(
            jax.ShapeDtypeStruct(density.shape, jnp.float32),
            jax.ShapeDtypeStruct((1, 1), jnp.float32),
        ),
        in_specs=in_vmem(2),
        out_specs=(
            pl.BlockSpec(memory_space=pltpu.VMEM),
            pl.BlockSpec(memory_space=pltpu.SMEM),
        ),
        compiler_params=params(12),
    )(got, deriv_z)
    return potential, energy.reshape(())


def solution(mesh):
    split = Mesh(mesh.devices.reshape((2,) * 7), GX + GY)
    return jax.shard_map(
        functools.partial(body, 256**3),
        mesh=split,
        in_specs=(P(GX, GY, None),),
        out_specs=(P(GX, GY, None), P()),
        check_vma=False,
    )
```

```python
import functools
import math

import jax
import jax.numpy as jnp
import numpy as np
from jax import lax
from jax.experimental import pallas as pl
from jax.experimental.pallas import tpu as pltpu
from jax.sharding import Mesh
from jax.sharding import PartitionSpec as P

GX = ("z1", "z0", "yh", "core")
GY = ("yl", "x1", "x0")
ORDER = ("core", "yh", "yl", "x1", "x0", "z1", "z0")
LANES = 128
VIEW = 8
BLOCK = 32

pbe_kappa = 0.804
pbe_mu = 0.2195149727645171
pbe_beta = 0.06672455060314922
pbe_gamma = 0.031090690869654894
pw_coef = 0.0310907
pw_alpha = 0.2137
pw_first = 7.5957
pw_second = 3.5876
pw_third = 1.6382
pw_fourth = 0.49294

fermi_scale = (3.0 * math.pi**2) ** (1.0 / 3.0)
exch_scale = 0.75 * fermi_scale / math.pi
s_scale = 1.0 / (4.0 * fermi_scale**2)
t_scale = math.pi / (16.0 * fermi_scale)
rs_scale = (3.0 / (4.0 * math.pi)) ** (1.0 / 3.0)
ex_scale = -exch_scale / rs_scale**2
root_slope = -1.0 / (6.0 * math.log(2.0))
root_shift = 0.5 * math.log2(rs_scale)
damping_scale = pbe_mu / pbe_kappa * s_scale / rs_scale**8
tau_scale = pbe_beta / pbe_gamma * t_scale / rs_scale**7
slope_scale = -2.0 * exch_scale * s_scale * pbe_mu / rs_scale**4
weight_scale = 2.0 * pbe_beta * t_scale / rs_scale**4
pw = [2.0 * pw_coef * factor for factor in (pw_first, pw_second, pw_third, pw_fourth)]


def deriv_matrix(count):
    index = np.arange(count)
    signed = np.where(index < count // 2, index, index - count)
    signed = np.where(index == count // 2, 0, signed)
    waves = signed * (2.0 * math.pi / count)
    phase = (index[:, None] * index[None, :] % count) * (2.0 * math.pi / count)
    cosine, sine = np.cos(phase), np.sin(phase)
    return ((cosine * waves) @ sine - (sine * waves) @ cosine) / count


def halves(values):
    high = values.astype(jnp.bfloat16)
    return high, (values - high.astype(jnp.float32)).astype(jnp.bfloat16)


def mul(left, right, axis=0):
    def dot(first, second):
        return lax.dot_general(
            first, second, (((1,), (axis,)), ((), ())), preferred_element_type=jnp.float32
        )

    return dot(left[0], right[0]) + dot(left[1], right[0]) + dot(left[0], right[1])


def pbe(n, g):
    root = jnp.exp2(jnp.log(n) * root_slope + root_shift)
    rs = root * root
    rs2 = rs * rs
    rs4 = rs2 * rs2
    scaled = g * rs4
    damping = 1.0 + damping_scale * (scaled * rs4)
    tau = tau_scale * (scaled * (rs2 * rs))
    part = n * rs2
    series = root * (pw[0] + root * (pw[1] + root * (pw[2] + root * pw[3])))
    third = root * (
        pw[0] / 6 + root * (pw[1] / 3 + root * (pw[2] / 2 + root * (pw[3] / 1.5)))
    )
    damp = 1.0 / damping
    flipped = 1.0 / series
    fraction = flipped * (1.0 / (1.0 + series))
    logarithm = jnp.log(1.0 + flipped)
    curved = (-2.0 * pw_coef * pw_alpha) * rs
    front = curved - 2.0 * pw_coef
    ec = front * logarithm
    n_dec = front * (third * fraction) - (curved * (1.0 / 3.0)) * logarithm
    grown = jnp.exp2(ec * (-1.0 / (pbe_gamma * math.log(2.0))))
    m = grown - 1.0
    m2 = m * m
    cross = tau * m
    tau2 = tau * tau
    near = m + tau
    base = m2 + cross + tau2
    top = base + cross * near
    lower = 1.0 / base
    both = lower * (1.0 / top)
    rest = ec + pbe_gamma * jnp.log(top * lower)
    damp2 = damp * damp
    energy = part * ((1.0 + pbe_kappa) * ex_scale - (pbe_kappa * ex_scale) * damp) + rest
    weight = (near + tau) * (m2 * m)
    twice = rs4 * (slope_scale * damp2 + (weight_scale * weight) * both)
    n_dh = (tau * both) * (
        (-7.0 / 3.0 * pbe_gamma) * weight - tau2 * ((near + m) * (grown * n_dec))
    )
    d_dens = (
        part
        * (
            (4.0 / 3.0) * (1.0 + pbe_kappa) * ex_scale
            + damp * ((-4.0 * pbe_kappa * ex_scale) + (8.0 / 3.0 * pbe_kappa * ex_scale) * damp)
        )
        + (rest + n_dec)
        + n_dh
    )
    return n * energy, d_dens, twice


def mix(parts, odd, upper):
    pairs = [jnp.where(odd, parts[(1 - t) % 4], parts[-t % 4]) for t in range(4)]
    return [jnp.where(upper, pairs[(t + 2) % 4], pairs[t]) for t in range(4)]


def place(a, b):
    at = {axis: a >> (3 - i) & 1 for i, axis in enumerate(GX)}
    at |= {axis: b >> (2 - i) & 1 for i, axis in enumerate(GY)}
    return functools.reduce(lambda index, axis: 2 * index + at[axis], ORDER, 0)


def masks():
    lane = lax.broadcasted_iota(jnp.int32, (VIEW, LANES), 1)
    row = lax.broadcasted_iota(jnp.int32, (VIEW, LANES), 0)
    return (lane & 32) != 0, (lane & 64) != 0, (row & 4) != 0


def turn():
    return 2 * lax.axis_index("x1") + lax.axis_index("x0")


def first_kernel(density_hbm, deriv_hbm, send_ref, density_ref, deriv_ref, wide_ref, sems):
    copies = [
        pltpu.make_async_copy(density_hbm, density_ref, sems.at[0]),
        pltpu.make_async_copy(deriv_hbm, deriv_ref, sems.at[1]),
    ]
    for copy in copies:
        copy.start()
    back = 4 - turn()
    for copy in copies:
        copy.wait()
    lines = jnp.concatenate(
        [density_ref[4 * (place // 4) + lax.rem(place % 4 + back, 4)] for place in range(16)]
    )
    turned = lines.T
    slopes = mul((deriv_ref[0], deriv_ref[1]), halves(lines), 1)
    rows = 2 * VIEW
    for field, values in enumerate((turned, slopes)):
        for plane in range(2):
            for part in range(4):
                row = VIEW * field + 4 * plane + part
                wide_ref[pl.ds(row, LANES, stride=rows + 1), :] = values[
                    LANES * plane : LANES * (plane + 1), LANES * part : LANES * (part + 1)
                ]
    for other in range(LANES):
        start = (rows + 1) * other
        send_ref[rows * other : rows * (other + 1), :] = wide_ref[start : start + rows, :]


def middle_kernel(
    got_ref, deriv_x_ref, deriv_y_ref, send_ref, dens_ref, grad_z_ref, grad_x_ref, grad_y_ref
):
    rows = 2 * VIEW
    odd, upper, below = masks()

    def receive(pair, field, ref):
        for half in range(2):
            for plane in range(2):
                parts = []
                for quarter in range(4):
                    block = 4 * half + quarter
                    shift = VIEW * field + 4 * plane
                    start = place(2 * pair, block) * rows + shift
                    later = place(2 * pair + 1, block) * rows + shift - 4
                    parts.append(
                        jnp.where(
                            below, got_ref[later : later + VIEW, :], got_ref[start : start + VIEW, :]
                        )
                    )
                for t, part in enumerate(mix(parts, odd, upper)):
                    start = (pair * 4 + t) * VIEW
                    ref[plane, start : start + VIEW, LANES * half : LANES * (half + 1)] = (
                        pltpu.roll(part, LANES - 32 * t, 1) if t else part
                    )

    def give(pair, field, ref):
        for half in range(2):
            for plane in range(2):
                parts = []
                for t in range(4):
                    start = (pair * 4 + t) * VIEW
                    part = ref[plane, start : start + VIEW, LANES * half : LANES * (half + 1)]
                    parts.append(pltpu.roll(part, 32 * t, 1) if t else part)
                for quarter, part in enumerate(mix(parts, odd, upper)):
                    block = 4 * half + quarter
                    shift = VIEW * field + 4 * plane
                    start = place(2 * pair, block) * (rows + 1) + shift
                    later = place(2 * pair + 1, block) * (rows + 1) + shift
                    send_ref[start : start + 4, :] = part[:4]
                    send_ref[later : later + 4, :] = part[4:]

    def slopes(plane):
        dens = halves(dens_ref[plane])
        grad_x_ref[plane] = mul((deriv_x_ref[0], deriv_x_ref[1]), dens)
        grad_y_ref[plane] = mul(dens, (deriv_y_ref[0], deriv_y_ref[1]))

    def subtract(plane):
        dens_ref[plane] = (
            dens_ref[plane]
            - mul((deriv_x_ref[0], deriv_x_ref[1]), halves(grad_x_ref[plane]))
            - mul(halves(grad_y_ref[plane]), (deriv_y_ref[0], deriv_y_ref[1]))
        )

    def evaluate(plane, total):
        for start in range(0, 256, BLOCK):
            block = plane, slice(start, start + BLOCK)
            n = dens_ref[block]
            gx, gy, gz = grad_x_ref[block], grad_y_ref[block], grad_z_ref[block]
            f, d_dens, twice = pbe(n, gx * gx + gy * gy + gz * gz)
            grad_x_ref[block] = twice * gx
            grad_y_ref[block] = twice * gy
            grad_z_ref[block] = twice * gz
            dens_ref[block] = d_dens
            total = total + f
        return total

    for pair in range(8):
        receive(pair, 0, dens_ref)
    slopes(0)
    for pair in range(8):
        receive(pair, 1, grad_z_ref)
    total = evaluate(0, jnp.zeros((BLOCK, 256), jnp.float32))
    slopes(1)
    subtract(0)
    total = evaluate(1, total)
    subtract(1)
    for pair in range(8):
        give(pair, 1, grad_z_ref)
    for pair in range(8):
        give(pair, 0, dens_ref)
    summed = jnp.sum(total[:, :LANES] + total[:, LANES:], axis=0, keepdims=True)
    send_ref[pl.ds(rows, LANES, stride=rows + 1), :] = jnp.broadcast_to(summed, (LANES, LANES))


def last_kernel(cells, got_ref, deriv_ref, potential_ref, energy_ref):
    rows = 2 * VIEW + 1
    back = 4 - turn()

    def gather(field):
        return jnp.concatenate(
            [
                jnp.concatenate(
                    [
                        got_ref[pl.ds(VIEW * field + 4 * plane + part, LANES, stride=rows), :]
                        for part in range(4)
                    ],
                    axis=1,
                )
                for plane in range(2)
            ],
            axis=0,
        )

    slopes = mul(halves(gather(1).T), (deriv_ref[0], deriv_ref[1]), 1)
    lines = gather(0).T - slopes
    for place in range(16):
        potential_ref[4 * (place // 4) + lax.rem(place % 4 + back, 4)] = lines[
            32 * place : 32 * (place + 1)
        ]
    energy_ref[0, 0] = jnp.sum(got_ref[pl.ds(rows - 1, LANES, stride=rows), :]) / cells


def params(megabytes):
    return pltpu.CompilerParams(vmem_limit_bytes=megabytes << 20)


def in_vmem(count):
    return [pl.BlockSpec(memory_space=pltpu.VMEM)] * count


def far(values):
    return pltpu.with_memory_space_constraint(values, pltpu.HBM)


def exchange(values):
    return lax.all_to_all(values, ORDER, split_axis=0, concat_axis=0, tiled=True)


def pair(matrix):
    high = matrix.astype(jnp.bfloat16)
    low = (matrix - high.astype(np.float64)).astype(jnp.bfloat16)
    return jnp.asarray(np.stack([high, low]))


def body(cells, density):
    count = density.shape[-1]
    deriv = deriv_matrix(count)
    row = np.arange(count)
    cell = 16 * (2 * (row // 32) + (row // 4) % 2) + 4 * (row % 4) + (row // 8) % 4
    deriv_z = pair(deriv)
    deriv_y = pair(deriv.T)
    deriv_x = pair(deriv[cell[:, None], cell[None, :]])

    send = pl.pallas_call(
        first_kernel,
        out_shape=jax.ShapeDtypeStruct((2048, LANES), jnp.float32),
        in_specs=[pl.BlockSpec(memory_space=pltpu.HBM)] * 2,
        out_specs=pl.BlockSpec(memory_space=pltpu.VMEM),
        scratch_shapes=[
            pltpu.VMEM(density.shape, jnp.float32),
            pltpu.VMEM((2, count, count), jnp.bfloat16),
            pltpu.VMEM((17 * LANES, LANES), jnp.float32),
            pltpu.SemaphoreType.DMA((2,)),
        ],
        compiler_params=params(12),
    )(far(density), far(deriv_z))
    got = exchange(send.reshape(LANES, 16, LANES)).reshape(2048, LANES)
    send = pl.pallas_call(
        middle_kernel,
        out_shape=jax.ShapeDtypeStruct((17 * LANES, LANES), jnp.float32),
        in_specs=in_vmem(3),
        out_specs=pl.BlockSpec(memory_space=pltpu.VMEM),
        scratch_shapes=[pltpu.VMEM((2, count, count), jnp.float32)] * 4,
        compiler_params=params(16),
    )(got, deriv_x, deriv_y)
    got = exchange(send.reshape(LANES, 1, 17 * LANES)).reshape(17 * LANES, LANES)
    potential, energy = pl.pallas_call(
        functools.partial(last_kernel, float(cells)),
        out_shape=(
            jax.ShapeDtypeStruct(density.shape, jnp.float32),
            jax.ShapeDtypeStruct((1, 1), jnp.float32),
        ),
        in_specs=in_vmem(2),
        out_specs=(
            pl.BlockSpec(memory_space=pltpu.VMEM),
            pl.BlockSpec(memory_space=pltpu.SMEM),
        ),
        compiler_params=params(12),
    )(got, deriv_z)
    return potential, energy.reshape(())


def solution(mesh):
    split = Mesh(mesh.devices.reshape((2,) * 7), GX + GY)
    return jax.shard_map(
        functools.partial(body, 256**3),
        mesh=split,
        in_specs=(P(GX, GY, None),),
        out_specs=(P(GX, GY, None), P()),
        check_vma=False,
    )
```

```python
import functools
import math

import jax
import jax.numpy as jnp
import numpy as np
from jax import lax
from jax.experimental import pallas as pl
from jax.experimental.pallas import tpu as pltpu
from jax.sharding import Mesh
from jax.sharding import PartitionSpec as P

GX = ("z1", "z0", "yh", "core")
GY = ("yl", "x1", "x0")
ORDER = ("core", "yh", "yl", "x1", "x0", "z1", "z0")
LANES = 128
VIEW = 8
BLOCK = 32

pbe_kappa = 0.804
pbe_mu = 0.2195149727645171
pbe_beta = 0.06672455060314922
pbe_gamma = 0.031090690869654894
pw_coef = 0.0310907
pw_alpha = 0.2137
pw_first = 7.5957
pw_second = 3.5876
pw_third = 1.6382
pw_fourth = 0.49294

fermi_scale = (3.0 * math.pi**2) ** (1.0 / 3.0)
exch_scale = 0.75 * fermi_scale / math.pi
s_scale = 1.0 / (4.0 * fermi_scale**2)
t_scale = math.pi / (16.0 * fermi_scale)
rs_scale = (3.0 / (4.0 * math.pi)) ** (1.0 / 3.0)
stretch = (pbe_mu / pbe_kappa * s_scale / rs_scale**8) ** (1.0 / 16.0)
ex_scale = -exch_scale / (rs_scale**2 * stretch**4)
root_slope = -1.0 / (6.0 * math.log(2.0))
root_shift = 0.5 * math.log2(rs_scale) + math.log2(stretch)
tau_scale = pbe_beta / pbe_gamma * t_scale / (rs_scale**7 * stretch**14)
slope_scale = -2.0 * exch_scale * s_scale * pbe_mu / (rs_scale**4 * stretch**8)
weight_scale = 2.0 * pbe_beta * t_scale / (rs_scale**4 * stretch**8)
pw = [
    2.0 * pw_coef * factor / stretch**power
    for power, factor in enumerate((pw_first, pw_second, pw_third, pw_fourth), 1)
]


def deriv_matrix(count):
    index = np.arange(count)
    signed = np.where(index < count // 2, index, index - count)
    signed = np.where(index == count // 2, 0, signed)
    waves = signed * (2.0 * math.pi / count)
    phase = (index[:, None] * index[None, :] % count) * (2.0 * math.pi / count)
    cosine, sine = np.cos(phase), np.sin(phase)
    return ((cosine * waves) @ sine - (sine * waves) @ cosine) / count


def halves(values):
    high = values.astype(jnp.bfloat16)
    return high, (values - high.astype(jnp.float32)).astype(jnp.bfloat16)


def mul(left, right, axis=0):
    def dot(first, second):
        return lax.dot_general(
            first, second, (((1,), (axis,)), ((), ())), preferred_element_type=jnp.float32
        )

    return dot(left[0], right[0]) + dot(left[1], right[0]) + dot(left[0], right[1])


def pbe(n, g):
    root = jnp.exp2(jnp.log(n) * root_slope + root_shift)
    rs = root * root
    rs2 = rs * rs
    rs4 = rs2 * rs2
    scaled = g * rs4
    damping = 1.0 + scaled * rs4
    tau = tau_scale * (scaled * (rs2 * rs))
    part = n * rs2
    series = root * (pw[0] + root * (pw[1] + root * (pw[2] + root * pw[3])))
    third = root * (
        pw[0] / 6 + root * (pw[1] / 3 + root * (pw[2] / 2 + root * (pw[3] / 1.5)))
    )
    damp = 1.0 / damping
    flipped = 1.0 / series
    fraction = flipped * (1.0 / (1.0 + series))
    logarithm = jnp.log(1.0 + flipped)
    curved = (-2.0 * pw_coef * pw_alpha / stretch**2) * rs
    front = curved - 2.0 * pw_coef
    ec = front * logarithm
    n_dec = front * (third * fraction) - (curved * (1.0 / 3.0)) * logarithm
    grown = jnp.exp2(ec * (-1.0 / (pbe_gamma * math.log(2.0))))
    m = grown - 1.0
    m2 = m * m
    cross = tau * m
    tau2 = tau * tau
    near = m + tau
    base = m2 + cross + tau2
    top = base + cross * near
    lower = 1.0 / base
    both = lower * (1.0 / top)
    rest = ec + pbe_gamma * jnp.log(top * lower)
    damp2 = damp * damp
    energy = part * ((1.0 + pbe_kappa) * ex_scale - (pbe_kappa * ex_scale) * damp) + rest
    weight = (near + tau) * (m2 * m)
    twice = rs4 * (slope_scale * damp2 + (weight_scale * weight) * both)
    n_dh = (tau * both) * (
        (-7.0 / 3.0 * pbe_gamma) * weight - tau2 * ((near + m) * (grown * n_dec))
    )
    d_dens = (
        part
        * (
            (4.0 / 3.0) * (1.0 + pbe_kappa) * ex_scale
            + damp * ((-4.0 * pbe_kappa * ex_scale) + (8.0 / 3.0 * pbe_kappa * ex_scale) * damp)
        )
        + (rest + n_dec)
        + n_dh
    )
    return n * energy, d_dens, twice


def mix(parts, odd, upper):
    pairs = [jnp.where(odd, parts[(1 - t) % 4], parts[-t % 4]) for t in range(4)]
    return [jnp.where(upper, pairs[(t + 2) % 4], pairs[t]) for t in range(4)]


def place(a, b):
    at = {axis: a >> (3 - i) & 1 for i, axis in enumerate(GX)}
    at |= {axis: b >> (2 - i) & 1 for i, axis in enumerate(GY)}
    return functools.reduce(lambda index, axis: 2 * index + at[axis], ORDER, 0)


def masks():
    lane = lax.broadcasted_iota(jnp.int32, (VIEW, LANES), 1)
    row = lax.broadcasted_iota(jnp.int32, (VIEW, LANES), 0)
    return (lane & 32) != 0, (lane & 64) != 0, (row & 4) != 0


def turn():
    return 2 * lax.axis_index("x1") + lax.axis_index("x0")


def first_kernel(density_hbm, deriv_hbm, send_ref, density_ref, deriv_ref, wide_ref, sems):
    copies = [
        pltpu.make_async_copy(density_hbm, density_ref, sems.at[0]),
        pltpu.make_async_copy(deriv_hbm, deriv_ref, sems.at[1]),
    ]
    for copy in copies:
        copy.start()
    back = 4 - turn()
    for copy in copies:
        copy.wait()
    lines = jnp.concatenate(
        [density_ref[4 * (place // 4) + lax.rem(place % 4 + back, 4)] for place in range(16)]
    )
    turned = lines.T
    slopes = mul((deriv_ref[0], deriv_ref[1]), halves(lines), 1)
    rows = 2 * VIEW
    for field, values in enumerate((turned, slopes)):
        for plane in range(2):
            for part in range(4):
                row = VIEW * field + 4 * plane + part
                wide_ref[pl.ds(row, LANES, stride=rows + 1), :] = values[
                    LANES * plane : LANES * (plane + 1), LANES * part : LANES * (part + 1)
                ]
    for other in range(LANES):
        start = (rows + 1) * other
        send_ref[rows * other : rows * (other + 1), :] = wide_ref[start : start + rows, :]


def middle_kernel(
    got_ref, deriv_x_ref, deriv_y_ref, send_ref, dens_ref, grad_z_ref, grad_x_ref, grad_y_ref
):
    rows = 2 * VIEW
    odd, upper, below = masks()

    def receive(pair, field, ref):
        for half in range(2):
            for plane in range(2):
                parts = []
                for quarter in range(4):
                    block = 4 * half + quarter
                    shift = VIEW * field + 4 * plane
                    start = place(2 * pair, block) * rows + shift
                    later = place(2 * pair + 1, block) * rows + shift - 4
                    parts.append(
                        jnp.where(
                            below, got_ref[later : later + VIEW, :], got_ref[start : start + VIEW, :]
                        )
                    )
                for t, part in enumerate(mix(parts, odd, upper)):
                    start = (pair * 4 + t) * VIEW
                    ref[plane, start : start + VIEW, LANES * half : LANES * (half + 1)] = (
                        pltpu.roll(part, LANES - 32 * t, 1) if t else part
                    )

    def give(pair, field, ref):
        for half in range(2):
            for plane in range(2):
                parts = []
                for t in range(4):
                    start = (pair * 4 + t) * VIEW
                    part = ref[plane, start : start + VIEW, LANES * half : LANES * (half + 1)]
                    parts.append(pltpu.roll(part, 32 * t, 1) if t else part)
                for quarter, part in enumerate(mix(parts, odd, upper)):
                    block = 4 * half + quarter
                    shift = VIEW * field + 4 * plane
                    start = place(2 * pair, block) * (rows + 1) + shift
                    later = place(2 * pair + 1, block) * (rows + 1) + shift
                    send_ref[start : start + 4, :] = part[:4]
                    send_ref[later : later + 4, :] = part[4:]

    def slopes(plane):
        dens = halves(dens_ref[plane])
        grad_x_ref[plane] = mul((deriv_x_ref[0], deriv_x_ref[1]), dens)
        grad_y_ref[plane] = mul(dens, (deriv_y_ref[0], deriv_y_ref[1]))

    def subtract(plane):
        dens_ref[plane] = (
            dens_ref[plane]
            - mul((deriv_x_ref[0], deriv_x_ref[1]), halves(grad_x_ref[plane]))
            - mul(halves(grad_y_ref[plane]), (deriv_y_ref[0], deriv_y_ref[1]))
        )

    def evaluate(plane, total):
        for start in range(0, 256, BLOCK):
            block = plane, slice(start, start + BLOCK)
            n = dens_ref[block]
            gx, gy, gz = grad_x_ref[block], grad_y_ref[block], grad_z_ref[block]
            f, d_dens, twice = pbe(n, gx * gx + gy * gy + gz * gz)
            grad_x_ref[block] = twice * gx
            grad_y_ref[block] = twice * gy
            grad_z_ref[block] = twice * gz
            dens_ref[block] = d_dens
            total = total + f
        return total

    for pair in range(8):
        receive(pair, 0, dens_ref)
    slopes(0)
    for pair in range(8):
        receive(pair, 1, grad_z_ref)
    total = evaluate(0, jnp.zeros((BLOCK, 256), jnp.float32))
    slopes(1)
    subtract(0)
    total = evaluate(1, total)
    subtract(1)
    for pair in range(8):
        give(pair, 1, grad_z_ref)
    for pair in range(8):
        give(pair, 0, dens_ref)
    summed = jnp.sum(total[:, :LANES] + total[:, LANES:], axis=0, keepdims=True)
    send_ref[pl.ds(rows, LANES, stride=rows + 1), :] = jnp.broadcast_to(summed, (LANES, LANES))


def last_kernel(cells, got_ref, deriv_ref, potential_ref, energy_ref):
    rows = 2 * VIEW + 1
    back = 4 - turn()

    def gather(field):
        return jnp.concatenate(
            [
                jnp.concatenate(
                    [
                        got_ref[pl.ds(VIEW * field + 4 * plane + part, LANES, stride=rows), :]
                        for part in range(4)
                    ],
                    axis=1,
                )
                for plane in range(2)
            ],
            axis=0,
        )

    slopes = mul(halves(gather(1).T), (deriv_ref[0], deriv_ref[1]), 1)
    lines = gather(0).T - slopes
    for place in range(16):
        potential_ref[4 * (place // 4) + lax.rem(place % 4 + back, 4)] = lines[
            32 * place : 32 * (place + 1)
        ]
    energy_ref[0, 0] = jnp.sum(got_ref[pl.ds(rows - 1, LANES, stride=rows), :]) / cells


def params(megabytes):
    return pltpu.CompilerParams(vmem_limit_bytes=megabytes << 20)


def in_vmem(count):
    return [pl.BlockSpec(memory_space=pltpu.VMEM)] * count


def far(values):
    return pltpu.with_memory_space_constraint(values, pltpu.HBM)


def exchange(values):
    return lax.all_to_all(values, ORDER, split_axis=0, concat_axis=0, tiled=True)


def pair(matrix):
    high = matrix.astype(jnp.bfloat16)
    low = (matrix - high.astype(np.float64)).astype(jnp.bfloat16)
    return jnp.asarray(np.stack([high, low]))


def body(cells, density):
    count = density.shape[-1]
    deriv = deriv_matrix(count)
    row = np.arange(count)
    cell = 16 * (2 * (row // 32) + (row // 4) % 2) + 4 * (row % 4) + (row // 8) % 4
    deriv_z = pair(deriv)
    deriv_y = pair(deriv.T)
    deriv_x = pair(deriv[cell[:, None], cell[None, :]])

    send = pl.pallas_call(
        first_kernel,
        out_shape=jax.ShapeDtypeStruct((2048, LANES), jnp.float32),
        in_specs=[pl.BlockSpec(memory_space=pltpu.HBM)] * 2,
        out_specs=pl.BlockSpec(memory_space=pltpu.VMEM),
        scratch_shapes=[
            pltpu.VMEM(density.shape, jnp.float32),
            pltpu.VMEM((2, count, count), jnp.bfloat16),
            pltpu.VMEM((17 * LANES, LANES), jnp.float32),
            pltpu.SemaphoreType.DMA((2,)),
        ],
        compiler_params=params(12),
    )(far(density), far(deriv_z))
    got = exchange(send.reshape(LANES, 16, LANES)).reshape(2048, LANES)
    send = pl.pallas_call(
        middle_kernel,
        out_shape=jax.ShapeDtypeStruct((17 * LANES, LANES), jnp.float32),
        in_specs=in_vmem(3),
        out_specs=pl.BlockSpec(memory_space=pltpu.VMEM),
        scratch_shapes=[pltpu.VMEM((2, count, count), jnp.float32)] * 4,
        compiler_params=params(16),
    )(got, deriv_x, deriv_y)
    got = exchange(send.reshape(LANES, 1, 17 * LANES)).reshape(17 * LANES, LANES)
    potential, energy = pl.pallas_call(
        functools.partial(last_kernel, float(cells)),
        out_shape=(
            jax.ShapeDtypeStruct(density.shape, jnp.float32),
            jax.ShapeDtypeStruct((1, 1), jnp.float32),
        ),
        in_specs=in_vmem(2),
        out_specs=(
            pl.BlockSpec(memory_space=pltpu.VMEM),
            pl.BlockSpec(memory_space=pltpu.SMEM),
        ),
        compiler_params=params(12),
    )(got, deriv_z)
    return potential, energy.reshape(())


def solution(mesh):
    split = Mesh(mesh.devices.reshape((2,) * 7), GX + GY)
    return jax.shard_map(
        functools.partial(body, 256**3),
        mesh=split,
        in_specs=(P(GX, GY, None),),
        out_specs=(P(GX, GY, None), P()),
        check_vma=False,
    )
```
